32 devices in a mesh: grp: 2 (over core), tile: 16 (over z, y, x).
Axes of the slice: x: 2, y: 2, z: 4, core: 2. Of those that a mesh axis runs over, the one named last changes fastest.
Arguments:
- source_points: float32 [2, 3, 524288], P('grp', None, 'tile'), may hold values from -6 to 6
- intersection: int32 [2, 2048, 1], P('grp', 'tile'), may hold values from 0 to 15; in each aligned block of 128 rows (0 to 127, 128 to 255, ..., all dimensions but the last counted through in order) at most 16 rows name the same one
- target_scan: int32 [2, 2048], P('grp', 'tile'), may hold values from 0 to 63
- matches: int32 [2, 524288], P('grp', 'tile'), may hold values from 0 to 511
- target_points: float32 [3, 524288], P(None, 'tile'), may hold values from -6 to 6
- target_normals: float32 [3, 524288], P(None, 'tile'), may hold values from -4 to 4
Outputs:
- pose_step: float32 [6, 1024], P(None, 'tile')
The draws below stay inside these ranges and needn't reach their ends.
Inputs may be any that keep to these rules, and one draw needn't show every extreme that they name: `intersection`: within the blocks of one device (each aligned run of 128 rows), no index is named more than 16 times, a bound that some block reaches.
All inputs are finite; a program needn't handle non-finite values.
Results may differ from the reference program's by a relative error of at most 0.0003.
Values sent between devices are 32-bit elements; how exact they have to be, the bound alone decides.
A program may use at most 64 MiB of HBM per device.

```python
import math
import jax
import jax.numpy as jnp
import numpy as np
from jax import lax

BLOCK_PTS = 256
BLOCKS_DEV = 128
SCANS_DEV = 64
TARGET_PTS = 512
CAP = 16
GRPS = 2
BLOCKS = 2048
SCANS = 1024
TILE_PTS = 524288
N_TILE = 16


def set_ends(array, stream_key, least, top_value):
    longest = array.shape.index(max(array.shape))
    spots = []
    for shift in (0, 1):
        where = [jax.random.randint(jax.random.fold_in(stream_key, axis), (), 0, length) for axis, length in enumerate(array.shape)]
        where[longest] = (where[longest] + shift) % array.shape[longest]
        spots.append(tuple(where))
    return array.at[spots[0]].set(least).at[spots[1]].set(top_value)


def shard_levels(stream_key, shape, shards, smallest, high):
    def one(axis_at, parts):
        steps = jax.random.uniform(jax.random.fold_in(jax.random.fold_in(stream_key, 6), axis_at), (parts,), jnp.float32, smallest / len(shards), high / len(shards))
        return jnp.repeat(jnp.exp(steps), shape[axis_at] // parts).reshape((-1,) + (1,) * (len(shape) - axis_at - 1))

    level = one(*shards[0])
    for cut in shards[1:]:
        level = level * one(*cut)
    return level


def routed_block(own_key, own, number, rows, amount, top, limit, skew):
    order = jax.random.permutation(own_key, amount)
    crowded, usual = shares(amount, rows * top, limit, skew, True), shares(amount, rows * top, limit, skew, False)
    places = jnp.arange(amount)

    def named(tallies, rotation):
        used = int((tallies > 0).sum())
        fixed = max(1, used // 4)
        passed = fixed + (places - fixed + rotation * (used - fixed)) % max(1, amount - fixed)
        return jnp.zeros((amount,), jnp.int32).at[order[jnp.where(places < fixed, places, passed)]].set(jnp.asarray(tallies, jnp.int32))

    tallies = jnp.where(number % 4 == 0, named(crowded, number // 4), named(usual, number - number // 4 - 1))
    mixed = jax.random.permutation(jax.random.fold_in(own, 3), amount)
    source_of, sink = mixed[0:amount // 2 * 2:2], mixed[1:amount // 2 * 2:2]
    slack = jnp.minimum(tallies[source_of] - 1, limit - tallies[sink]) // 2
    slack = jnp.where((source_of == order[0]) | (sink == order[0]) | (tallies[sink] == 0), 0, jnp.maximum(slack, 0))
    passed = jax.random.randint(jax.random.fold_in(own, 4), (amount // 2,), 0, 1 << 20) % (slack + 1)
    tallies = tallies.at[source_of].add(-passed).at[sink].add(passed)
    members = jnp.searchsorted(jnp.cumsum(tallies), jnp.arange(rows * top), side="right").astype(jnp.int32)
    grid = members.reshape(top, rows).T
    grid = grid[jax.random.permutation(jax.random.fold_in(own, 1), rows)]
    rotation = jax.random.randint(jax.random.fold_in(own, 2), (rows, 1), 0, top)
    return jnp.take_along_axis(grid, (jnp.arange(top)[None, :] + rotation) % top, axis=1)


def shares(amount, total, most, lean, full):
    loads = [(1 << 20) // math.isqrt(grade ** lean) + 1 for grade in range(1, amount + 1)]
    largest = most if full else min(most, max(-(-total // amount), total * loads[0] // sum(loads)))
    least = 1 if total - largest >= amount - 1 else 0
    given, spare = [largest] + [least] * (amount - 1), total - largest - least * (amount - 1)
    while spare > 0:
        movable = [i for i in range(1, amount) if given[i] < largest] or [i for i in range(1, amount) if given[i] < most]
        pool, left = sum([loads[i] for i in movable]), spare
        for i in movable:
            more = min(most - given[i], max(1, left * loads[i] // pool), spare)
            given[i] = given[i] + more
            spare = spare - more
    return np.array(given)


def gaussian(key, extent, width, reach, pieces=(), kind=jnp.bfloat16):
    drawn = jax.random.normal(key, extent, jnp.float32) * width
    if len(pieces) > 0:
        drawn = shard_levels(key, extent, pieces, -0.22, 0.18) * drawn
    return jnp.clip(drawn, min=-reach, max=reach).astype(kind)


def setup_inputs(seed: int = 0) -> dict:
    keys = jax.random.split(jax.random.key(seed), 7)
    source_points = gaussian(keys[0], (GRPS, 3, BLOCKS * BLOCK_PTS), 1.0, 6.0, ((0, 2), (2, 16)), jnp.float32)
    intersection_keys = jax.random.split(jax.random.fold_in(keys[1], 1), GRPS * BLOCKS // BLOCKS_DEV)
    intersection_turns = jax.random.permutation(jax.random.fold_in(keys[1], 3), GRPS * BLOCKS // BLOCKS_DEV)
    intersection = jax.vmap(lambda own, number: routed_block(jax.random.fold_in(keys[1], 2), own, number, BLOCKS_DEV, N_TILE, 1, CAP, 2))(intersection_keys, intersection_turns).reshape((GRPS, BLOCKS, 1))
    target_scan = set_ends(jax.random.randint(keys[2], (GRPS, BLOCKS), 0, SCANS_DEV), jax.random.fold_in(keys[2], 1), 0, SCANS_DEV - 1).astype(jnp.int32)
    matches = set_ends(jax.random.randint(keys[3], (GRPS, BLOCKS * BLOCK_PTS), 0, TARGET_PTS), jax.random.fold_in(keys[3], 1), 0, TARGET_PTS - 1).astype(jnp.int32)
    target_points = gaussian(keys[4], (3, TILE_PTS), 1.0, 6.0, ((1, 16),), jnp.float32)
    target_normals = gaussian(keys[5], (3, TILE_PTS), 0.6, 4.0, ((1, 16),), jnp.float32)
    return {"source_points": source_points, "intersection": intersection, "target_scan": target_scan, "matches": matches, "target_points": target_points, "target_normals": target_normals}


DAMPING = 0.1
PRECISE = lax.Precision.HIGHEST


def cross_rows(first_vec, second_vec):
    return jnp.stack([first_vec[1] * second_vec[2] - first_vec[2] * second_vec[1],
                      first_vec[2] * second_vec[0] - first_vec[0] * second_vec[2],
                      first_vec[0] * second_vec[1] - first_vec[1] * second_vec[0]])


def pair_terms(source, target, normal, usable):
    jacobian = jnp.concatenate([cross_rows(source, normal), normal, -cross_rows(target, normal), -normal], axis=0) * usable[None]
    misfit = jnp.sum(normal * (source - target), axis=0) * usable
    normal_blocks = jnp.einsum("anks,bnks->abnk", jacobian, jacobian, precision=PRECISE)
    gradient = jnp.einsum("anks,nks->ank", jacobian, misfit, precision=PRECISE)
    layout = jacobian.shape[1:3]
    own_terms = jnp.concatenate([normal_blocks[:6, :6].reshape((36,) + layout), gradient[:6]], axis=0)
    theirs = jnp.concatenate([normal_blocks[6:, 6:].reshape((36,) + layout), gradient[6:]], axis=0)
    return own_terms, theirs


def solve_poses(scan_totals):
    entries = [[scan_totals[6 * row_at + col_at] for col_at in range(6)] for row_at in range(6)]
    traced = entries[0][0]
    for step_at in range(1, 6):
        traced = traced + entries[step_at][step_at]
    shift_by = DAMPING * traced / 6.0
    for step_at in range(6):
        entries[step_at][step_at] = entries[step_at][step_at] + shift_by
    values = [-scan_totals[36 + row_at] for row_at in range(6)]
    for pivot_at in range(6):
        for row_at in range(pivot_at + 1, 6):
            factor = entries[row_at][pivot_at] / entries[pivot_at][pivot_at]
            for col_at in range(pivot_at, 6):
                entries[row_at][col_at] = entries[row_at][col_at] - factor * entries[pivot_at][col_at]
            values[row_at] = values[row_at] - factor * values[pivot_at]
    result = [None] * 6
    for row_at in range(5, -1, -1):
        running = values[row_at]
        for col_at in range(row_at + 1, 6):
            running = running - entries[row_at][col_at] * result[col_at]
        result[row_at] = running / entries[row_at][row_at]
    return jnp.stack(result)


def reference(source_points, intersection, target_scan, matches, target_points, target_normals):
    per_scan = BLOCKS_DEV // SCANS_DEV
    block_span = BLOCKS_DEV * BLOCK_PTS
    tile_span = SCANS_DEV * TARGET_PTS
    anchor = jnp.int32(0)

    def accumulate(totals, stretch_at):
        grp_at = (stretch_at // N_TILE).astype(jnp.int32)
        tile_at = (stretch_at % N_TILE).astype(jnp.int32)
        coords = lax.dynamic_slice(source_points, (grp_at, anchor, tile_at * block_span), (1, 3, block_span))[0]
        coords = coords.reshape(3, 1, BLOCKS_DEV, BLOCK_PTS)
        destin = lax.dynamic_slice(intersection, (grp_at, tile_at * BLOCKS_DEV, anchor), (1, BLOCKS_DEV, 1))[0, :, 0]
        chosen = lax.dynamic_slice(target_scan, (grp_at, tile_at * BLOCKS_DEV), (1, BLOCKS_DEV))[0]
        picked = lax.dynamic_slice(matches, (grp_at, tile_at * block_span), (1, block_span))[0].reshape(BLOCKS_DEV, BLOCK_PTS)
        target_index = (destin[:, None] * tile_span + chosen[:, None] * TARGET_PTS + picked).astype(jnp.int32)
        nearest = jnp.take(target_points, target_index, axis=1)[:, None]
        facing = jnp.take(target_normals, target_index, axis=1)[:, None]
        usable = jnp.ones((1, BLOCKS_DEV, BLOCK_PTS), jnp.float32)
        own_terms, theirs = pair_terms(coords, nearest, facing, usable)
        source_ids = (tile_at * SCANS_DEV + jnp.arange(BLOCKS_DEV, dtype=jnp.int32) // per_scan).astype(jnp.int32)
        target_ids = (destin * SCANS_DEV + chosen).astype(jnp.int32)
        totals = totals + jax.ops.segment_sum(own_terms[:, 0].T, source_ids, num_segments=SCANS).T
        totals = totals + jax.ops.segment_sum(theirs[:, 0].T, target_ids, num_segments=SCANS).T
        return totals, None

    totals, unused = lax.scan(accumulate, jnp.zeros((42, SCANS), jnp.float32), jnp.arange(GRPS * N_TILE, dtype=jnp.int32))
    return solve_poses(totals)
```

```python
import functools

import jax
import jax.numpy as jnp
from jax import lax
from jax.experimental import pallas as pl
from jax.experimental.pallas import tpu as pltpu
from jax.sharding import PartitionSpec as P

SCANS_DEV = 64
TARGET_PTS = 512
DAMPING = 0.1
LANES = 128
PRECISE = lax.Precision.HIGHEST
MESH = pl.DeviceIdType.MESH
VMEM = pl.BlockSpec(memory_space=pltpu.VMEM)
SMEM = pl.BlockSpec(memory_space=pltpu.SMEM)


def pack_kernel(dest, chosen, sp, mt, pts, idx, seg, count):
    tiles, _, cap, points = pts.shape
    blocks = dest.shape[0]
    per_scan = blocks // SCANS_DEV
    idx[...] = jnp.full(idx.shape, -1, jnp.int32)

    def clear(t, c):
        count[t] = 0
        return c

    lax.fori_loop(0, tiles, clear, 0)

    def unset(s, c):
        seg[0, s] = -1
        return c

    lax.fori_loop(0, tiles * cap, unset, 0, unroll=8)

    def step(b, c):
        d = dest[b]
        r = count[d]
        count[d] = r + 1
        seg[0, d * cap + r] = b // per_scan
        cols = pl.ds(pl.multiple_of(b * points, points), points)
        for a in range(3):
            pts[d, a, pl.ds(r, 1), :] = sp[0, a : a + 1, cols]
        idx[d, pl.ds(r, 1), :] = mt[0:1, cols] + chosen[0, b] * TARGET_PTS
        return c

    lax.fori_loop(0, blocks, step, 0, unroll=4)


def greet_tiles(tiles, me, extra):
    barrier = pltpu.get_barrier_semaphore()

    def one(k, c):
        pl.semaphore_signal(
            barrier, inc=1, device_id={"tile": lax.rem(me + k, tiles)}, device_id_type=MESH
        )
        return c

    lax.fori_loop(1, tiles, one, 0)
    if extra:
        pl.semaphore_signal(
            barrier, inc=1, device_id={"grp": 1 - lax.axis_index("grp")}, device_id_type=MESH
        )
    pl.semaphore_wait(barrier, tiles - 1 + extra)


def exchange_kernel(pts, idx, got_pts, got_idx, ps, pr, qs, qr, ls):
    tiles = pts.shape[0]
    me = lax.axis_index("tile")
    greet_tiles(tiles, me, 0)

    def copies(to, frm):
        return (
            pltpu.make_async_remote_copy(
                idx.at[to], got_idx.at[frm], qs.at[to], qr.at[frm], {"tile": to}, MESH
            ),
            pltpu.make_async_remote_copy(
                pts.at[to], got_pts.at[frm], ps.at[to], pr.at[frm], {"tile": to}, MESH
            ),
        )

    def send(k, c):
        for copy in copies(lax.rem(me + k, tiles), me):
            copy.start()
        return c

    lax.fori_loop(1, tiles, send, 0)
    mine = (
        pltpu.make_async_copy(idx.at[me], got_idx.at[me], ls.at[0]),
        pltpu.make_async_copy(pts.at[me], got_pts.at[me], ls.at[1]),
    )
    for copy in mine:
        copy.start()
    for copy in mine:
        copy.wait()

    def finish(k, c):
        to = lax.rem(me + k, tiles)
        frm = lax.rem(me + tiles - k, tiles)
        for copy in copies(to, frm):
            copy.wait_send()
        for copy in copies(to, frm):
            copy.wait_recv()
        return c

    lax.fori_loop(1, tiles, finish, 0)


def cross(u, v):
    return [
        u[1] * v[2] - u[2] * v[1],
        u[2] * v[0] - u[0] * v[2],
        u[0] * v[1] - u[1] * v[0],
    ]


def upper(vec):
    return [(a, b) for a in range(6) for b in range(a, 6)]


def compute_kernel(ids, pts, idx, tp, tn, own, far, table, picked):
    tiles, _, cap, points = pts.shape

    def fill(s, c):
        cols = pl.ds(pl.multiple_of(s * TARGET_PTS, TARGET_PTS), TARGET_PTS)
        table[s, 0:3, :] = tp[:, cols]
        table[s, 3:6, :] = tn[:, cols]
        return c

    lax.fori_loop(0, SCANS_DEV, fill, 0, unroll=4)
    lane = lax.broadcasted_iota(jnp.int32, (8, LANES), 1)

    def group(i, c):
        d = i // (cap // 8)
        r0 = pl.multiple_of((i % (cap // 8)) * 8, 8)
        near = idx[d, pl.ds(r0, 8), :]
        for j in range(8):
            tab = table.at[jnp.maximum(ids[i * 8 + j], 0)]
            for h in range(points // LANES):
                at = jnp.broadcast_to(near[j : j + 1, h * LANES : (h + 1) * LANES], (8, LANES))
                low = at & (LANES - 1)
                high = (at >> 7) & (TARGET_PTS // LANES - 1)
                out = None
                for q in range(TARGET_PTS // LANES):
                    part = jnp.take_along_axis(
                        tab[:, q * LANES : (q + 1) * LANES],
                        low,
                        axis=1,
                        mode="promise_in_bounds",
                    )
                    out = part if out is None else jnp.where(high == q, part, out)
                picked[h, j * 8 : j * 8 + 8, :] = out
        halves = []
        for h in range(points // LANES):
            span = slice(h * LANES, (h + 1) * LANES)
            good = near[:, span] >= 0
            p = [jnp.where(good, pts[d, a, pl.ds(r0, 8), span], 0.0) for a in range(3)]
            q = [picked[h, pl.ds(a, 8, stride=8), :] for a in range(3)]
            n = [
                jnp.where(good, picked[h, pl.ds(3 + a, 8, stride=8), :], 0.0) for a in range(3)
            ]
            mis = n[0] * (p[0] - q[0]) + n[1] * (p[1] - q[1]) + n[2] * (p[2] - q[2])
            halves.append((cross(p, n) + n, cross(q, n) + n, mis))
        own_row = jnp.zeros((8, LANES), jnp.float32)
        far_row = jnp.zeros((8, LANES), jnp.float32)

        def total(make):
            acc = None
            for half in halves:
                acc = make(half) if acc is None else acc + make(half)
            return jnp.sum(acc, axis=1, keepdims=True)

        for f, (a, b) in enumerate(upper(6)):
            s = total(lambda v: v[0][a] * v[0][b])
            own_row = jnp.where(lane == f, s, own_row)
            if a < 3:
                s = total(lambda v: v[1][a] * v[1][b])
            far_row = jnp.where(lane == f, s, far_row)
        for a in range(6):
            s = total(lambda v: v[0][a] * v[2])
            own_row = jnp.where(lane == 21 + a, s, own_row)
            if a < 3:
                s = total(lambda v: v[1][a] * v[2])
            far_row = jnp.where(lane == 21 + a, -s, far_row)
        own[d, pl.ds(r0, 8), :] = own_row
        far[d, pl.ds(r0, 8), :] = far_row
        return c

    lax.fori_loop(0, tiles * (cap // 8), group, 0)


def solve_rows(rows):
    entries = {}
    for f, (a, b) in enumerate(upper(6)):
        entries[a, b] = rows[f]
    traced = entries[0, 0]
    for a in range(1, 6):
        traced = traced + entries[a, a]
    shift_by = DAMPING * traced / 6.0
    for a in range(6):
        entries[a, a] = entries[a, a] + shift_by
    values = [-rows[21 + a] for a in range(6)]
    for k in range(6):
        for a in range(k + 1, 6):
            factor = entries[k, a] / entries[k, k]
            for b in range(a, 6):
                entries[a, b] = entries[a, b] - factor * entries[k, b]
            values[a] = values[a] - factor * values[k]
    result = [None] * 6
    for a in range(5, -1, -1):
        running = values[a]
        for b in range(a + 1, 6):
            running = running - entries[a, b] * result[b]
        result[a] = running / entries[a, a]
    return result


def return_kernel(own, far, seg, ids, out, back, tot, partner, ss, rs, gs, gr):
    tiles, cap, _ = own.shape
    me = lax.axis_index("tile")
    greet_tiles(tiles, me, 1)

    def copy(to, frm):
        return pltpu.make_async_remote_copy(
            own.at[to], back.at[frm], ss.at[to], rs.at[frm], {"tile": to}, MESH
        )

    def send(k, c):
        copy(lax.rem(me + k, tiles), me).start()
        return c

    lax.fori_loop(1, tiles, send, 0)
    back[me] = own[me]
    scan = lax.broadcasted_iota(jnp.int32, (SCANS_DEV, tiles * cap), 0)
    to_far = (scan == ids[...]).astype(jnp.float32)
    to_own = (scan == seg[...]).astype(jnp.float32)
    sums = jnp.dot(
        to_far,
        far[...].reshape(tiles * cap, LANES),
        precision=PRECISE,
        preferred_element_type=jnp.float32,
    )

    def finish(k, c):
        copy(lax.rem(me + k, tiles), lax.rem(me + tiles - k, tiles)).wait()
        return c

    lax.fori_loop(1, tiles, finish, 0)
    sums = sums + jnp.dot(
        to_own,
        back[...].reshape(tiles * cap, LANES),
        precision=PRECISE,
        preferred_element_type=jnp.float32,
    )
    tot[...] = sums
    swap = pltpu.make_async_remote_copy(
        tot, partner, gs, gr, {"grp": 1 - lax.axis_index("grp")}, MESH
    )
    swap.start()
    swap.wait()
    full = jnp.transpose(tot[...] + partner[...])
    for a, row in enumerate(solve_rows([full[f : f + 1, :] for f in range(27)])):
        out[a : a + 1, :] = row


def body(source_points, intersection, target_scan, matches, target_points, target_normals):
    tiles = lax.axis_size("tile")
    blocks = intersection.shape[1]
    points = source_points.shape[2] // blocks
    cap = -(-(2 * blocks // tiles) // 8) * 8
    f32, i32 = jnp.float32, jnp.int32
    shape = jax.ShapeDtypeStruct
    dma = pltpu.SemaphoreType.DMA
    pts, idx, seg = pl.pallas_call(
        pack_kernel,
        out_shape=(
            shape((tiles, 3, cap, points), f32),
            shape((tiles, cap, points), i32),
            shape((1, tiles * cap), i32),
        ),
        in_specs=[SMEM, SMEM, VMEM, VMEM],
        out_specs=(VMEM, VMEM, SMEM),
        scratch_shapes=[pltpu.SMEM((tiles,), i32)],
        name="pack",
    )(intersection.reshape(blocks), target_scan, source_points, matches)
    pts, idx = pl.pallas_call(
        exchange_kernel,
        out_shape=(shape(pts.shape, f32), shape(idx.shape, i32)),
        in_specs=[VMEM, VMEM],
        out_specs=(VMEM, VMEM),
        scratch_shapes=[dma((tiles,)), dma((tiles,)), dma((tiles,)), dma((tiles,)), dma((2,))],
        compiler_params=pltpu.CompilerParams(collective_id=0, has_side_effects=True),
        name="exchange",
    )(pts, idx)
    lead = idx[:, :, 0].reshape(1, tiles * cap)
    ids = jnp.where(lead >= 0, lead // TARGET_PTS, -1)
    own, far = pl.pallas_call(
        compute_kernel,
        out_shape=(shape((tiles, cap, LANES), f32), shape((tiles, cap, LANES), f32)),
        in_specs=[SMEM, VMEM, VMEM, VMEM, VMEM],
        out_specs=(VMEM, VMEM),
        scratch_shapes=[
            pltpu.VMEM((SCANS_DEV, 8, TARGET_PTS), f32),
            pltpu.VMEM((points // LANES, 64, LANES), f32),
        ],
        name="compute",
    )(ids.reshape(tiles * cap), pts, idx, target_points, target_normals)
    return pl.pallas_call(
        return_kernel,
        out_shape=shape((6, SCANS_DEV), f32),
        in_specs=[VMEM, VMEM, VMEM, VMEM],
        out_specs=VMEM,
        scratch_shapes=[
            pltpu.VMEM((tiles, cap, LANES), f32),
            pltpu.VMEM((SCANS_DEV, LANES), f32),
            pltpu.VMEM((SCANS_DEV, LANES), f32),
            dma((tiles,)),
            dma((tiles,)),
            dma,
            dma,
        ],
        compiler_params=pltpu.CompilerParams(collective_id=1, has_side_effects=True),
        name="giveback",
    )(own, far, seg, ids)


def solution(mesh):
    in_specs = (
        P("grp", None, "tile"),
        P("grp", "tile", None),
        P("grp", "tile"),
        P("grp", "tile"),
        P(None, "tile"),
        P(None, "tile"),
    )
    out_specs = P(None, "tile")
    return jax.shard_map(body, mesh=mesh, in_specs=in_specs, out_specs=out_specs, check_vma=False)
```

```python
import jax
import jax.numpy as jnp
from jax import lax
from jax.experimental import pallas as pl
from jax.experimental.pallas import tpu as pltpu
from jax.sharding import PartitionSpec as P

SCANS_DEV = 64
TARGET_PTS = 512
DAMPING = 0.1
LANES = 128
PAIR = 32
PRECISE = lax.Precision.HIGHEST
MESH = pl.DeviceIdType.MESH
VMEM = pl.BlockSpec(memory_space=pltpu.VMEM)
SMEM = pl.BlockSpec(memory_space=pltpu.SMEM)


def pack_kernel(dest, chosen, sp, mt, pts, idx, ids, seg, count):
    tiles, _, cap, points = pts.shape
    blocks = dest.shape[0]
    per_scan = blocks // SCANS_DEV
    idx[...] = jnp.full(idx.shape, -1, jnp.int32)

    def clear(t, c):
        count[t] = 0
        for r in range(cap):
            ids[t, 0, r] = -1
            seg[r // 8, t * 8 + r % 8] = -1
        return c

    lax.fori_loop(0, tiles, clear, 0)

    def step(b, c):
        d = dest[b]
        r = count[d]
        count[d] = r + 1
        seg[r // 8, d * 8 + r % 8] = b // per_scan
        ids[d, 0, r] = chosen[0, b]
        cols = pl.ds(pl.multiple_of(b * points, points), points)
        for a in range(3):
            pts[d, a, pl.ds(r, 1), :] = sp[0, a : a + 1, cols]
        idx[d, pl.ds(r, 1), :] = mt[0:1, cols]
        return c

    lax.fori_loop(0, blocks, step, 0, unroll=4)


def near_first(tiles, me, start, act):
    def one(j, c):
        k = (j + 1) // 2
        t = me + k * (2 * (j % 2) - 1)

        @pl.when((t >= 0) & (t < tiles))
        def _():
            act(t, j)

        return c

    lax.fori_loop(start, 2 * tiles - 1, one, 0)


def cross(u, v):
    return [
        u[1] * v[2] - u[2] * v[1],
        u[2] * v[0] - u[0] * v[2],
        u[0] * v[1] - u[1] * v[0],
    ]


def upper(vec):
    return [(a, b) for a in range(6) for b in range(a, 6)]


def main_kernel(
    pts, idx, ids, seg, tp, tn, out,
    got_pts, got_idx, got_ids, named, table, picked, own, far, back, tot, partner,
    ps, pr, qs, qr, js, jr, ss, rs, ls, gs, gr,
):
    tiles, _, cap, points = pts.shape
    me = lax.axis_index("tile")
    other = 1 - lax.axis_index("grp")
    barrier = pltpu.get_barrier_semaphore()

    def greet(k, c):
        to = lax.rem(me + k, tiles)
        pl.semaphore_signal(barrier, inc=1, device_id={"tile": to}, device_id_type=MESH)
        return c

    lax.fori_loop(1, tiles, greet, 0)
    pl.semaphore_signal(barrier, inc=1, device_id={"grp": other}, device_id_type=MESH)
    pl.semaphore_wait(barrier, tiles)

    def remote(src, dst, send, recv, to, frm):
        return pltpu.make_async_remote_copy(
            src.at[to], dst.at[frm], send.at[to], recv.at[frm], {"tile": to}, MESH
        )

    def id_copy(to, frm):
        return remote(ids, got_ids, js, jr, to, frm)

    def idx_copy(to, frm):
        return remote(idx, got_idx, qs, qr, to, frm)

    def pts_copy(to, frm):
        return remote(pts, got_pts, ps, pr, to, frm)

    def own_copy(to, frm):
        return remote(own, back, ss, rs, to, frm)

    near_first(tiles, me, 1, lambda t, j: id_copy(t, me).start())

    def send(t, j):
        idx_copy(t, me).start()
        pts_copy(t, me).start()

    near_first(tiles, me, 1, send)
    mine = [
        pltpu.make_async_copy(src.at[me], dst.at[me], ls.at[i])
        for i, (src, dst) in enumerate(((ids, got_ids), (idx, got_idx), (pts, got_pts)))
    ]
    for copy in mine:
        copy.start()

    def fill(s, c):
        cols = pl.ds(pl.multiple_of(s * TARGET_PTS, TARGET_PTS), TARGET_PTS)
        table[s, 0:3, :] = tp[:, cols]
        table[s, 3:6, :] = tn[:, cols]
        return c

    lax.fori_loop(0, SCANS_DEV, fill, 0, unroll=4)
    tot[...] = jnp.zeros(tot.shape, jnp.float32)
    for copy in mine:
        copy.wait()
    near_first(tiles, me, 1, lambda t, j: id_copy(t, t).wait_recv())
    load_ids = pltpu.make_async_copy(got_ids, named, ls.at[3])
    load_ids.start()
    load_ids.wait()
    lane = lax.broadcasted_iota(jnp.int32, (8, LANES), 1)
    scan = lax.broadcasted_iota(jnp.int32, (SCANS_DEV, cap), 0)

    def group(d, g):
        r0 = g * 8
        near = got_idx[d, r0 : r0 + 8, :]
        for j in range(8):
            tab = table.at[jnp.maximum(named[d, 0, r0 + j], 0)]
            for h in range(points // LANES):
                at = jnp.broadcast_to(near[j : j + 1, h * LANES : (h + 1) * LANES], (8, LANES))
                low = at & (LANES - 1)
                high = (at >> 7) & (TARGET_PTS // LANES - 1)
                res = None
                for q in range(TARGET_PTS // LANES):
                    part = jnp.take_along_axis(
                        tab[:, q * LANES : (q + 1) * LANES],
                        low,
                        axis=1,
                        mode="promise_in_bounds",
                    )
                    res = part if res is None else jnp.where(high == q, part, res)
                picked[g, h, j * 8 : j * 8 + 8, :] = res
        halves = []
        for h in range(points // LANES):
            span = slice(h * LANES, (h + 1) * LANES)
            good = near[:, span] >= 0
            p = [
                jnp.where(good, got_pts[d, a, r0 : r0 + 8, span], 0.0) for a in range(3)
            ]
            q = [picked[g, h, pl.ds(a, 8, stride=8), :] for a in range(3)]
            n = [
                jnp.where(good, picked[g, h, pl.ds(3 + a, 8, stride=8), :], 0.0)
                for a in range(3)
            ]
            mis = n[0] * (p[0] - q[0]) + n[1] * (p[1] - q[1]) + n[2] * (p[2] - q[2])
            halves.append((cross(p, n) + n, cross(q, n) + n, mis))
        own_row = jnp.zeros((8, LANES), jnp.float32)
        far_row = jnp.zeros((8, LANES), jnp.float32)

        def total(make):
            acc = None
            for half in halves:
                acc = make(half) if acc is None else acc + make(half)
            return jnp.sum(acc, axis=1, keepdims=True)

        for f, (a, b) in enumerate(upper(6)):
            s = total(lambda v: v[0][a] * v[0][b])
            own_row = jnp.where(lane == PAIR * g + f, s, own_row)
            if a < 3:
                s = total(lambda v: v[1][a] * v[1][b])
            far_row = jnp.where(lane == f, s, far_row)
        for a in range(6):
            s = total(lambda v: v[0][a] * v[2])
            own_row = jnp.where(lane == PAIR * g + 21 + a, s, own_row)
            if a < 3:
                s = total(lambda v: v[1][a] * v[2])
            far_row = jnp.where(lane == 21 + a, -s, far_row)
        far[r0 : r0 + 8, :] = far_row
        return own_row

    def work(t, j):
        @pl.when(j > 0)
        def _():
            idx_copy(t, t).wait_recv()
            pts_copy(t, t).wait_recv()

        row = group(t, 0)
        for g in range(1, cap // 8):
            row = row + group(t, g)
        own[t] = row

        @pl.when(j == 0)
        def _():
            back[me] = own[me]

        @pl.when(j > 0)
        def _():
            own_copy(t, me).start()

        here = (scan == got_ids[t][:, :cap]).astype(jnp.float32)
        tot[...] += jnp.dot(
            here, far[...], precision=PRECISE, preferred_element_type=jnp.float32
        )

    near_first(tiles, me, 0, work)
    near_first(tiles, me, 1, lambda t, j: own_copy(t, t).wait_recv())
    wide = lax.broadcasted_iota(jnp.int32, (SCANS_DEV, tiles * 8), 0)
    rows = back[...].reshape(tiles * 8, LANES)
    sums = tot[...]
    for g in range(cap // 8):
        here = (wide == seg[g : g + 1, :]).astype(jnp.float32)
        part = jnp.dot(here, rows, precision=PRECISE, preferred_element_type=jnp.float32)
        if g > 0:
            part = pltpu.roll(part, LANES - PAIR * g, 1)
        sums = sums + part
    tot[...] = sums
    swap = pltpu.make_async_remote_copy(tot, partner, gs, gr, {"grp": other}, MESH)
    swap.start()

    def drain(t, j):
        for copy in (id_copy, idx_copy, pts_copy, own_copy):
            copy(t, me).wait_send()

    near_first(tiles, me, 1, drain)
    swap.wait()
    out[...] = jnp.transpose(tot[...] + partner[...])[:PAIR]


def solve_rows(rows):
    entries = {}
    for f, (a, b) in enumerate(upper(6)):
        entries[a, b] = rows[f]
    traced = entries[0, 0]
    for a in range(1, 6):
        traced = traced + entries[a, a]
    shift_by = DAMPING * traced / 6.0
    for a in range(6):
        entries[a, a] = entries[a, a] + shift_by
    values = [-rows[21 + a] for a in range(6)]
    for k in range(6):
        for a in range(k + 1, 6):
            factor = entries[k, a] / entries[k, k]
            for b in range(a, 6):
                entries[a, b] = entries[a, b] - factor * entries[k, b]
            values[a] = values[a] - factor * values[k]
    result = [None] * 6
    for a in range(5, -1, -1):
        running = values[a]
        for b in range(a + 1, 6):
            running = running - entries[a, b] * result[b]
        result[a] = running / entries[a, a]
    return result


def body(source_points, intersection, target_scan, matches, target_points, target_normals):
    tiles = lax.axis_size("tile")
    blocks = intersection.shape[1]
    points = source_points.shape[2] // blocks
    cap = -(-(2 * blocks // tiles) // 8) * 8
    f32, i32 = jnp.float32, jnp.int32
    shape = jax.ShapeDtypeStruct
    many = pltpu.SemaphoreType.DMA((tiles,))
    pts_t, idx_t = (tiles, 3, cap, points), (tiles, cap, points)
    ids_t, sums_t = (tiles, 1, LANES), (SCANS_DEV, LANES)
    pts, idx, ids, seg = pl.pallas_call(
        pack_kernel,
        out_shape=(
            shape(pts_t, f32),
            shape(idx_t, i32),
            shape(ids_t, i32),
            shape((cap // 8, tiles * 8), i32),
        ),
        in_specs=[SMEM, SMEM, VMEM, VMEM],
        out_specs=(VMEM, VMEM, SMEM, SMEM),
        scratch_shapes=[pltpu.SMEM((tiles,), i32)],
        name="pack",
    )(intersection.reshape(blocks), target_scan, source_points, matches)
    rows = pl.pallas_call(
        main_kernel,
        out_shape=shape((PAIR, SCANS_DEV), f32),
        in_specs=[VMEM] * 6,
        out_specs=VMEM,
        scratch_shapes=[
            pltpu.VMEM(pts_t, f32),
            pltpu.VMEM(idx_t, i32),
            pltpu.VMEM(ids_t, i32),
            pltpu.SMEM(ids_t, i32),
            pltpu.VMEM((SCANS_DEV, 8, TARGET_PTS), f32),
            pltpu.VMEM((cap // 8, points // LANES, 64, LANES), f32),
            pltpu.VMEM((tiles, 8, LANES), f32),
            pltpu.VMEM((cap, LANES), f32),
            pltpu.VMEM((tiles, 8, LANES), f32),
            pltpu.VMEM(sums_t, f32),
            pltpu.VMEM(sums_t, f32),
        ]
        + [many] * 8
        + [pltpu.SemaphoreType.DMA((4,)), pltpu.SemaphoreType.DMA, pltpu.SemaphoreType.DMA],
        compiler_params=pltpu.CompilerParams(collective_id=0, has_side_effects=True),
        name="main",
    )(pts, idx, ids, seg, target_points, target_normals)
    return jnp.stack(solve_rows(rows))


def solution(mesh):
    in_specs = (
        P("grp", None, "tile"),
        P("grp", "tile", None),
        P("grp", "tile"),
        P("grp", "tile"),
        P(None, "tile"),
        P(None, "tile"),
    )
    out_specs = P(None, "tile")
    return jax.shard_map(body, mesh=mesh, in_specs=in_specs, out_specs=out_specs, check_vma=False)
```

```python
import jax
import jax.numpy as jnp
from jax import lax
from jax.experimental import pallas as pl
from jax.experimental.pallas import tpu as pltpu
from jax.sharding import PartitionSpec as P

SCANS_DEV = 64
TARGET_PTS = 512
DAMPING = 0.1
LANES = 128
PAIR = 32
PRECISE = lax.Precision.HIGHEST
MESH = pl.DeviceIdType.MESH
VMEM = pl.BlockSpec(memory_space=pltpu.VMEM)
SMEM = pl.BlockSpec(memory_space=pltpu.SMEM)


def plan_kernel(dest, chosen, block, ids, seg, count):
    tiles = ids.shape[0]
    blocks = dest.shape[0]
    cap = block.shape[0] // tiles
    per_scan = blocks // SCANS_DEV

    def clear(t, c):
        count[t] = 0
        for r in range(cap):
            block[t * cap + r] = -1
            ids[t, 0, r] = -1
            seg[r // 8, t * 8 + r % 8] = -1
        return c

    lax.fori_loop(0, tiles, clear, 0)

    def step(b, c):
        d = dest[b]
        r = count[d]
        count[d] = r + 1
        seg[r // 8, d * 8 + r % 8] = b // per_scan
        ids[d, 0, r] = chosen[0, b]
        block[d * cap + r] = b
        return c

    lax.fori_loop(0, blocks, step, 0, unroll=4)


def near_first(tiles, me, start, act):
    def one(j, c):
        k = (j + 1) // 2
        t = me + k * (2 * (j % 2) - 1)

        @pl.when((t >= 0) & (t < tiles))
        def _():
            act(t, j)

        return c

    lax.fori_loop(start, 2 * tiles - 1, one, 0)


def cross(u, v):
    return [
        u[1] * v[2] - u[2] * v[1],
        u[2] * v[0] - u[0] * v[2],
        u[0] * v[1] - u[1] * v[0],
    ]


def upper(vec):
    return [(a, b) for a in range(6) for b in range(a, 6)]


def main_kernel(
    block, sp, mt, ids, seg, tp, tn, out,
    pts, idx, got_pts, got_idx, got_ids, named, table, picked, own, far, back, tot, partner,
    ps, pr, qs, qr, js, jr, ss, rs, ls, gs, gr,
):
    tiles, _, cap, points = pts.shape
    me = lax.axis_index("tile")
    other = 1 - lax.axis_index("grp")
    barrier = pltpu.get_barrier_semaphore()

    def greet(k, c):
        to = lax.rem(me + k, tiles)
        pl.semaphore_signal(barrier, inc=1, device_id={"tile": to}, device_id_type=MESH)
        return c

    lax.fori_loop(1, tiles, greet, 0)
    pl.semaphore_signal(barrier, inc=1, device_id={"grp": other}, device_id_type=MESH)
    pl.semaphore_wait(barrier, tiles)

    def remote(src, dst, send, recv, to, frm):
        return pltpu.make_async_remote_copy(
            src.at[to], dst.at[frm], send.at[to], recv.at[frm], {"tile": to}, MESH
        )

    def id_copy(to, frm):
        return remote(ids, got_ids, js, jr, to, frm)

    def idx_copy(to, frm):
        return remote(idx, got_idx, qs, qr, to, frm)

    def pts_copy(to, frm):
        return remote(pts, got_pts, ps, pr, to, frm)

    def own_copy(to, frm):
        return remote(own, back, ss, rs, to, frm)

    near_first(tiles, me, 1, lambda t, j: id_copy(t, me).start())

    def pack(t, pts_to, idx_to):
        for r in range(cap):
            b = block[t * cap + r]
            used = jnp.minimum(b, 0) + 1
            for h in range(points // LANES):
                span = slice(h * LANES, (h + 1) * LANES)
                at = jnp.maximum(b, 0) * (points // LANES) + h
                for a in range(3):
                    pts_to[t, a, r : r + 1, span] = sp[a, at]
                idx_to[t, r : r + 1, span] = mt[at] * used + (used - 1)

    def at_step(j):
        return me + (j + 1) // 2 * (2 * (j % 2) - 1)

    def pack_send(j, c):
        t = at_step(j)

        @pl.when((j < 2 * tiles - 1) & (t >= 0) & (t < tiles))
        def _():
            pack(t, pts, idx)

        u = at_step(j - 1)

        @pl.when((j > 1) & (u >= 0) & (u < tiles))
        def _():
            idx_copy(u, me).start()
            pts_copy(u, me).start()

        return c

    lax.fori_loop(1, 2 * tiles, pack_send, 0)
    self_ids = pltpu.make_async_copy(ids.at[me], got_ids.at[me], ls.at[0])
    self_ids.start()
    pack(me, got_pts, got_idx)

    def fill(s, c):
        cols = pl.ds(pl.multiple_of(s * TARGET_PTS, TARGET_PTS), TARGET_PTS)
        table[s, 0:3, :] = tp[:, cols]
        table[s, 3:6, :] = tn[:, cols]
        return c

    lax.fori_loop(0, SCANS_DEV, fill, 0, unroll=4)
    tot[...] = jnp.zeros(tot.shape, jnp.float32)
    self_ids.wait()
    near_first(tiles, me, 1, lambda t, j: id_copy(t, t).wait_recv())
    load_ids = pltpu.make_async_copy(got_ids, named, ls.at[1])
    load_ids.start()
    load_ids.wait()
    lane = lax.broadcasted_iota(jnp.int32, (8, LANES), 1)
    scan = lax.broadcasted_iota(jnp.int32, (SCANS_DEV, cap), 0)

    def group(d, g):
        r0 = g * 8
        near = got_idx[d, r0 : r0 + 8, :]
        for j in range(8):
            tab = table.at[jnp.maximum(named[d, 0, r0 + j], 0)]
            for h in range(points // LANES):
                at = jnp.broadcast_to(near[j : j + 1, h * LANES : (h + 1) * LANES], (8, LANES))
                low = at & (LANES - 1)
                high = (at >> 7) & (TARGET_PTS // LANES - 1)
                res = None
                for q in range(TARGET_PTS // LANES):
                    part = jnp.take_along_axis(
                        tab[:, q * LANES : (q + 1) * LANES],
                        low,
                        axis=1,
                        mode="promise_in_bounds",
                    )
                    res = part if res is None else jnp.where(high == q, part, res)
                picked[g, h, j * 8 : j * 8 + 8, :] = res
        halves = []
        for h in range(points // LANES):
            span = slice(h * LANES, (h + 1) * LANES)
            good = near[:, span] >= 0
            p = [
                jnp.where(good, got_pts[d, a, r0 : r0 + 8, span], 0.0) for a in range(3)
            ]
            q = [picked[g, h, pl.ds(a, 8, stride=8), :] for a in range(3)]
            n = [
                jnp.where(good, picked[g, h, pl.ds(3 + a, 8, stride=8), :], 0.0)
                for a in range(3)
            ]
            mis = n[0] * (p[0] - q[0]) + n[1] * (p[1] - q[1]) + n[2] * (p[2] - q[2])
            halves.append((cross(p, n) + n, cross(q, n) + n, mis))
        own_row = jnp.zeros((8, LANES), jnp.float32)
        far_row = jnp.zeros((8, LANES), jnp.float32)

        def total(make):
            acc = None
            for half in halves:
                acc = make(half) if acc is None else acc + make(half)
            return jnp.sum(acc, axis=1, keepdims=True)

        for f, (a, b) in enumerate(upper(6)):
            s = total(lambda v: v[0][a] * v[0][b])
            own_row = jnp.where(lane == PAIR * g + f, s, own_row)
            if a < 3:
                s = total(lambda v: v[1][a] * v[1][b])
            far_row = jnp.where(lane == f, s, far_row)
        for a in range(6):
            s = total(lambda v: v[0][a] * v[2])
            own_row = jnp.where(lane == PAIR * g + 21 + a, s, own_row)
            if a < 3:
                s = total(lambda v: v[1][a] * v[2])
            far_row = jnp.where(lane == 21 + a, -s, far_row)
        far[r0 : r0 + 8, :] = far_row
        return own_row

    def work(t, j):
        @pl.when(j > 0)
        def _():
            idx_copy(t, t).wait_recv()
            pts_copy(t, t).wait_recv()

        row = group(t, 0)
        for g in range(1, cap // 8):
            row = row + group(t, g)
        own[t] = row

        @pl.when(j == 0)
        def _():
            back[me] = own[me]

        @pl.when(j > 0)
        def _():
            own_copy(t, me).start()

        here = (scan == got_ids[t][:, :cap]).astype(jnp.float32)
        tot[...] += jnp.dot(
            here, far[...], precision=PRECISE, preferred_element_type=jnp.float32
        )

    near_first(tiles, me, 0, work)
    near_first(tiles, me, 1, lambda t, j: own_copy(t, t).wait_recv())
    wide = lax.broadcasted_iota(jnp.int32, (SCANS_DEV, tiles * 8), 0)
    rows = back[...].reshape(tiles * 8, LANES)
    sums = tot[...]
    for g in range(cap // 8):
        here = (wide == seg[g : g + 1, :]).astype(jnp.float32)
        part = jnp.dot(here, rows, precision=PRECISE, preferred_element_type=jnp.float32)
        if g > 0:
            part = pltpu.roll(part, LANES - PAIR * g, 1)
        sums = sums + part
    tot[...] = sums
    swap = pltpu.make_async_remote_copy(tot, partner, gs, gr, {"grp": other}, MESH)
    swap.start()

    def drain(t, j):
        for copy in (id_copy, idx_copy, pts_copy, own_copy):
            copy(t, me).wait_send()

    near_first(tiles, me, 1, drain)
    swap.wait()
    full = jnp.transpose(tot[...] + partner[...])
    for a, row in enumerate(solve_rows([full[f : f + 1, :] for f in range(27)])):
        out[a : a + 1, :] = row


def solve_rows(rows):
    entries = {}
    for f, (a, b) in enumerate(upper(6)):
        entries[a, b] = rows[f]
    traced = entries[0, 0]
    for a in range(1, 6):
        traced = traced + entries[a, a]
    shift_by = DAMPING * traced / 6.0
    for a in range(6):
        entries[a, a] = entries[a, a] + shift_by
    values = [-rows[21 + a] for a in range(6)]
    for k in range(6):
        for a in range(k + 1, 6):
            factor = entries[k, a] / entries[k, k]
            for b in range(a, 6):
                entries[a, b] = entries[a, b] - factor * entries[k, b]
            values[a] = values[a] - factor * values[k]
    result = [None] * 6
    for a in range(5, -1, -1):
        running = values[a]
        for b in range(a + 1, 6):
            running = running - entries[a, b] * result[b]
        result[a] = running / entries[a, a]
    return result


def body(source_points, intersection, target_scan, matches, target_points, target_normals):
    tiles = lax.axis_size("tile")
    blocks = intersection.shape[1]
    points = source_points.shape[2] // blocks
    cap = -(-(2 * blocks // tiles) // 8) * 8
    f32, i32 = jnp.float32, jnp.int32
    shape = jax.ShapeDtypeStruct
    many = pltpu.SemaphoreType.DMA((tiles,))
    pts_t, idx_t = (tiles, 3, cap, points), (tiles, cap, points)
    ids_t, sums_t = (tiles, 1, LANES), (SCANS_DEV, LANES)
    block, ids, seg = pl.pallas_call(
        plan_kernel,
        out_shape=(
            shape((tiles * cap,), i32),
            shape(ids_t, i32),
            shape((cap // 8, tiles * 8), i32),
        ),
        in_specs=[SMEM, SMEM],
        out_specs=(SMEM, SMEM, SMEM),
        scratch_shapes=[pltpu.SMEM((tiles,), i32)],
        name="plan",
    )(intersection.reshape(blocks), target_scan)
    return pl.pallas_call(
        main_kernel,
        out_shape=shape((6, SCANS_DEV), f32),
        in_specs=[SMEM] + [VMEM] * 6,
        out_specs=VMEM,
        scratch_shapes=[
            pltpu.VMEM(pts_t, f32),
            pltpu.VMEM(idx_t, i32),
            pltpu.VMEM(pts_t, f32),
            pltpu.VMEM(idx_t, i32),
            pltpu.VMEM(ids_t, i32),
            pltpu.SMEM(ids_t, i32),
            pltpu.VMEM((SCANS_DEV, 8, TARGET_PTS), f32),
            pltpu.VMEM((cap // 8, points // LANES, 64, LANES), f32),
            pltpu.VMEM((tiles, 8, LANES), f32),
            pltpu.VMEM((cap, LANES), f32),
            pltpu.VMEM((tiles, 8, LANES), f32),
            pltpu.VMEM(sums_t, f32),
            pltpu.VMEM(sums_t, f32),
        ]
        + [many] * 8
        + [pltpu.SemaphoreType.DMA((2,)), pltpu.SemaphoreType.DMA, pltpu.SemaphoreType.DMA],
        compiler_params=pltpu.CompilerParams(collective_id=0, has_side_effects=True),
        name="main",
    )(
        block,
        source_points.reshape(3, -1, 1, LANES),
        matches.reshape(-1, 1, LANES),
        ids,
        seg,
        target_points,
        target_normals,
    )


def solution(mesh):
    in_specs = (
        P("grp", None, "tile"),
        P("grp", "tile", None),
        P("grp", "tile"),
        P("grp", "tile"),
        P(None, "tile"),
        P(None, "tile"),
    )
    out_specs = P(None, "tile")
    return jax.shard_map(body, mesh=mesh, in_specs=in_specs, out_specs=out_specs, check_vma=False)
```

```python
import jax
import jax.numpy as jnp
from jax import lax
from jax.experimental import pallas as pl
from jax.experimental.pallas import tpu as pltpu
from jax.sharding import PartitionSpec as P

SCANS_DEV = 64
TARGET_PTS = 512
DAMPING = 0.1
LANES = 128
PAIR = 32
PRECISE = lax.Precision.HIGHEST
MESH = pl.DeviceIdType.MESH
VMEM = pl.BlockSpec(memory_space=pltpu.VMEM)
SMEM = pl.BlockSpec(memory_space=pltpu.SMEM)


def plan_kernel(dest, chosen, block, ids, seg):
    tiles = ids.shape[0]
    blocks = dest.shape[1]
    cap = seg.shape[0] * 8
    per_scan = blocks // SCANS_DEV
    f32 = jnp.float32
    hit = dest[...] == lax.broadcasted_iota(jnp.int32, (tiles, blocks), 0)
    first = lax.broadcasted_iota(jnp.int32, (blocks, blocks), 0)
    second = lax.broadcasted_iota(jnp.int32, (blocks, blocks), 1)
    rank = jnp.dot(
        hit.astype(f32), (first <= second).astype(f32), preferred_element_type=f32
    ).astype(jnp.int32)
    rank = jnp.where(hit, rank, 0)
    place = lax.broadcasted_iota(jnp.int32, (tiles, blocks), 1).astype(f32) + 1.0
    wanted = chosen[...].astype(f32) + 1.0
    lane = lax.broadcasted_iota(jnp.int32, (tiles, LANES), 1)
    at = jnp.zeros((tiles, LANES), f32)
    named = jnp.zeros((tiles, LANES), f32)
    for r in range(cap):
        mine = rank == r + 1
        at = jnp.where(
            lane == r, jnp.sum(jnp.where(mine, place, 0.0), axis=1, keepdims=True), at
        )
        named = jnp.where(
            lane == r, jnp.sum(jnp.where(mine, wanted, 0.0), axis=1, keepdims=True), named
        )
    at = at.astype(jnp.int32) - 1
    named = named.astype(jnp.int32) - 1
    block[...] = at
    scan = jnp.where(at >= 0, at // per_scan, -1)
    for t in range(tiles):
        ids[t] = named[t : t + 1]
    for g in range(cap // 8):
        seg[g : g + 1, :] = jnp.concatenate(
            [scan[t : t + 1, g * 8 : g * 8 + 8] for t in range(tiles)], axis=1
        )


def near_first(tiles, me, start, act):
    def one(j, c):
        k = (j + 1) // 2
        t = me + k * (2 * (j % 2) - 1)

        @pl.when((t >= 0) & (t < tiles))
        def _():
            act(t, j)

        return c

    lax.fori_loop(start, 2 * tiles - 1, one, 0)


def cross(u, v):
    return [
        u[1] * v[2] - u[2] * v[1],
        u[2] * v[0] - u[0] * v[2],
        u[0] * v[1] - u[1] * v[0],
    ]


def upper(vec):
    return [(a, b) for a in range(6) for b in range(a, 6)]


def main_kernel(
    block, sp, mt, ids, seg, tp, tn, out,
    pts, idx, got_pts, got_idx, got_ids, named, table, picked, own, far, back, tot, partner,
    ps, pr, qs, qr, js, jr, ss, rs, ls, gs, gr,
):
    tiles, _, cap, points = pts.shape
    me = lax.axis_index("tile")
    other = 1 - lax.axis_index("grp")
    barrier = pltpu.get_barrier_semaphore()

    def greet(k, c):
        to = lax.rem(me + k, tiles)
        pl.semaphore_signal(barrier, inc=1, device_id={"tile": to}, device_id_type=MESH)
        return c

    lax.fori_loop(1, tiles, greet, 0)
    pl.semaphore_signal(barrier, inc=1, device_id={"grp": other}, device_id_type=MESH)
    pl.semaphore_wait(barrier, tiles)

    def remote(src, dst, send, recv, to, frm):
        return pltpu.make_async_remote_copy(
            src.at[to], dst.at[frm], send.at[to], recv.at[frm], {"tile": to}, MESH
        )

    def id_copy(to, frm):
        return remote(ids, got_ids, js, jr, to, frm)

    def idx_copy(to, frm):
        return remote(idx, got_idx, qs, qr, to, frm)

    def pts_copy(to, frm):
        return remote(pts, got_pts, ps, pr, to, frm)

    def own_copy(to, frm):
        return remote(own, back, ss, rs, to, frm)

    near_first(tiles, me, 1, lambda t, j: id_copy(t, me).start())

    def pack(t, pts_to, idx_to):
        for r in range(cap):
            b = block[t, r]
            used = jnp.minimum(b, 0) + 1
            for h in range(points // LANES):
                span = slice(h * LANES, (h + 1) * LANES)
                at = jnp.maximum(b, 0) * (points // LANES) + h
                for a in range(3):
                    pts_to[t, a, r : r + 1, span] = sp[a, at]
                idx_to[t, r : r + 1, span] = mt[at] * used + (used - 1)

    def at_step(j):
        return me + (j + 1) // 2 * (2 * (j % 2) - 1)

    def pack_send(j, c):
        t = at_step(j)

        @pl.when((j < 2 * tiles - 1) & (t >= 0) & (t < tiles))
        def _():
            pack(t, pts, idx)

        u = at_step(j - 1)

        @pl.when((j > 1) & (u >= 0) & (u < tiles))
        def _():
            idx_copy(u, me).start()
            pts_copy(u, me).start()

        return c

    lax.fori_loop(1, 2 * tiles, pack_send, 0)
    self_ids = pltpu.make_async_copy(ids.at[me], got_ids.at[me], ls.at[0])
    self_ids.start()
    pack(me, got_pts, got_idx)

    def fill(s, c):
        cols = pl.ds(pl.multiple_of(s * TARGET_PTS, TARGET_PTS), TARGET_PTS)
        table[s, 0:3, :] = tp[:, cols]
        table[s, 3:6, :] = tn[:, cols]
        return c

    lax.fori_loop(0, SCANS_DEV, fill, 0, unroll=4)
    tot[...] = jnp.zeros(tot.shape, jnp.float32)
    self_ids.wait()
    near_first(tiles, me, 1, lambda t, j: id_copy(t, t).wait_recv())
    load_ids = pltpu.make_async_copy(got_ids, named, ls.at[1])
    load_ids.start()
    load_ids.wait()
    lane = lax.broadcasted_iota(jnp.int32, (8, LANES), 1)
    scan = lax.broadcasted_iota(jnp.int32, (SCANS_DEV, cap), 0)

    def group(d, g):
        r0 = g * 8
        near = got_idx[d, r0 : r0 + 8, :]
        for j in range(8):
            tab = table.at[jnp.maximum(named[d, 0, r0 + j], 0)]
            for h in range(points // LANES):
                at = jnp.broadcast_to(near[j : j + 1, h * LANES : (h + 1) * LANES], (8, LANES))
                low = at & (LANES - 1)
                high = (at >> 7) & (TARGET_PTS // LANES - 1)
                res = None
                for q in range(TARGET_PTS // LANES):
                    part = jnp.take_along_axis(
                        tab[:, q * LANES : (q + 1) * LANES],
                        low,
                        axis=1,
                        mode="promise_in_bounds",
                    )
                    res = part if res is None else jnp.where(high == q, part, res)
                picked[g, h, j * 8 : j * 8 + 8, :] = res
        halves = []
        for h in range(points // LANES):
            span = slice(h * LANES, (h + 1) * LANES)
            good = near[:, span] >= 0
            p = [
                jnp.where(good, got_pts[d, a, r0 : r0 + 8, span], 0.0) for a in range(3)
            ]
            q = [picked[g, h, pl.ds(a, 8, stride=8), :] for a in range(3)]
            n = [
                jnp.where(good, picked[g, h, pl.ds(3 + a, 8, stride=8), :], 0.0)
                for a in range(3)
            ]
            mis = n[0] * (p[0] - q[0]) + n[1] * (p[1] - q[1]) + n[2] * (p[2] - q[2])
            halves.append((cross(p, n) + n, cross(q, n) + n, mis))
        own_row = jnp.zeros((8, LANES), jnp.float32)
        far_row = jnp.zeros((8, LANES), jnp.float32)

        def total(make):
            acc = None
            for half in halves:
                acc = make(half) if acc is None else acc + make(half)
            return jnp.sum(acc, axis=1, keepdims=True)

        for f, (a, b) in enumerate(upper(6)):
            s = total(lambda v: v[0][a] * v[0][b])
            own_row = jnp.where(lane == PAIR * g + f, s, own_row)
            if a < 3:
                s = total(lambda v: v[1][a] * v[1][b])
            far_row = jnp.where(lane == f, s, far_row)
        for a in range(6):
            s = total(lambda v: v[0][a] * v[2])
            own_row = jnp.where(lane == PAIR * g + 21 + a, s, own_row)
            if a < 3:
                s = total(lambda v: v[1][a] * v[2])
            far_row = jnp.where(lane == 21 + a, -s, far_row)
        far[r0 : r0 + 8, :] = far_row
        return own_row

    def work(t, j):
        @pl.when(j > 0)
        def _():
            idx_copy(t, t).wait_recv()
            pts_copy(t, t).wait_recv()

        row = group(t, 0)
        for g in range(1, cap // 8):
            row = row + group(t, g)
        own[t] = row

        @pl.when(j == 0)
        def _():
            back[me] = own[me]

        @pl.when(j > 0)
        def _():
            own_copy(t, me).start()

        here = (scan == got_ids[t][:, :cap]).astype(jnp.float32)
        tot[...] += jnp.dot(
            here, far[...], precision=PRECISE, preferred_element_type=jnp.float32
        )

    near_first(tiles, me, 0, work)
    near_first(tiles, me, 1, lambda t, j: own_copy(t, t).wait_recv())
    wide = lax.broadcasted_iota(jnp.int32, (SCANS_DEV, tiles * 8), 0)
    rows = back[...].reshape(tiles * 8, LANES)
    sums = tot[...]
    for g in range(cap // 8):
        here = (wide == seg[g : g + 1, :]).astype(jnp.float32)
        part = jnp.dot(here, rows, precision=PRECISE, preferred_element_type=jnp.float32)
        if g > 0:
            part = pltpu.roll(part, LANES - PAIR * g, 1)
        sums = sums + part
    tot[...] = sums
    swap = pltpu.make_async_remote_copy(tot, partner, gs, gr, {"grp": other}, MESH)
    swap.start()

    def drain(t, j):
        for copy in (id_copy, idx_copy, pts_copy, own_copy):
            copy(t, me).wait_send()

    near_first(tiles, me, 1, drain)
    swap.wait()
    full = jnp.transpose(tot[...] + partner[...])
    for a, row in enumerate(solve_rows([full[f : f + 1, :] for f in range(27)])):
        out[a : a + 1, :] = row


def solve_rows(rows):
    entries = {}
    for f, (a, b) in enumerate(upper(6)):
        entries[a, b] = rows[f]
    traced = entries[0, 0]
    for a in range(1, 6):
        traced = traced + entries[a, a]
    shift_by = DAMPING * traced / 6.0
    for a in range(6):
        entries[a, a] = entries[a, a] + shift_by
    values = [-rows[21 + a] for a in range(6)]
    for k in range(6):
        for a in range(k + 1, 6):
            factor = entries[k, a] / entries[k, k]
            for b in range(a, 6):
                entries[a, b] = entries[a, b] - factor * entries[k, b]
            values[a] = values[a] - factor * values[k]
    result = [None] * 6
    for a in range(5, -1, -1):
        running = values[a]
        for b in range(a + 1, 6):
            running = running - entries[a, b] * result[b]
        result[a] = running / entries[a, a]
    return result


def body(source_points, intersection, target_scan, matches, target_points, target_normals):
    tiles = lax.axis_size("tile")
    blocks = intersection.shape[1]
    points = source_points.shape[2] // blocks
    cap = -(-(2 * blocks // tiles) // 8) * 8
    f32, i32 = jnp.float32, jnp.int32
    shape = jax.ShapeDtypeStruct
    many = pltpu.SemaphoreType.DMA((tiles,))
    pts_t, idx_t = (tiles, 3, cap, points), (tiles, cap, points)
    ids_t, sums_t = (tiles, 1, LANES), (SCANS_DEV, LANES)
    block, ids, seg = pl.pallas_call(
        plan_kernel,
        out_shape=(
            shape((tiles, LANES), i32),
            shape(ids_t, i32),
            shape((cap // 8, tiles * 8), i32),
        ),
        in_specs=[VMEM, VMEM],
        out_specs=(VMEM, VMEM, VMEM),
        name="plan",
    )(intersection.reshape(1, blocks), target_scan)
    return pl.pallas_call(
        main_kernel,
        out_shape=shape((6, SCANS_DEV), f32),
        in_specs=[SMEM] + [VMEM] * 6,
        out_specs=VMEM,
        scratch_shapes=[
            pltpu.VMEM(pts_t, f32),
            pltpu.VMEM(idx_t, i32),
            pltpu.VMEM(pts_t, f32),
            pltpu.VMEM(idx_t, i32),
            pltpu.VMEM(ids_t, i32),
            pltpu.SMEM(ids_t, i32),
            pltpu.VMEM((SCANS_DEV, 8, TARGET_PTS), f32),
            pltpu.VMEM((cap // 8, points // LANES, 64, LANES), f32),
            pltpu.VMEM((tiles, 8, LANES), f32),
            pltpu.VMEM((cap, LANES), f32),
            pltpu.VMEM((tiles, 8, LANES), f32),
            pltpu.VMEM(sums_t, f32),
            pltpu.VMEM(sums_t, f32),
        ]
        + [many] * 8
        + [pltpu.SemaphoreType.DMA((2,)), pltpu.SemaphoreType.DMA, pltpu.SemaphoreType.DMA],
        compiler_params=pltpu.CompilerParams(collective_id=0, has_side_effects=True),
        name="main",
    )(
        block,
        source_points.reshape(3, -1, 1, LANES),
        matches.reshape(-1, 1, LANES),
        ids,
        seg,
        target_points,
        target_normals,
    )


def solution(mesh):
    in_specs = (
        P("grp", None, "tile"),
        P("grp", "tile", None),
        P("grp", "tile"),
        P("grp", "tile"),
        P(None, "tile"),
        P(None, "tile"),
    )
    out_specs = P(None, "tile")
    return jax.shard_map(body, mesh=mesh, in_specs=in_specs, out_specs=out_specs, check_vma=False)
```
